32 devices in a mesh: gx: 2 (over y), gy: 4 (over x, core), gz: 4 (over z).
Axes of the slice: x: 2, y: 2, z: 4, core: 2. Of those that a mesh axis runs over, the one named last changes fastest.
Arguments:
- species: float32 [5, 8, 32, 512], P(None, 'gx', 'gy', 'gz'), may hold values from 0.09 to 0.6
- velocity_in: float32 [3, 8, 32, 512], P(None, 'gx', 'gy', 'gz'), may hold values from -3 to 3
- pressure_in: float32 [8, 32, 512], P('gx', 'gy', 'gz'), may hold values from 0.125 to 1
- wall_types: int32 [3, 2, 8, 128], P(None, 'gx', 'gy', 'gz'), may hold values 0 or 1
Outputs:
- new_state: float32 [9, 8, 32, 512], P(None, 'gx', 'gy', 'gz')
- blending: float32 [2, 8, 128], P('gx', 'gy', 'gz')
The draws below stay inside these ranges and needn't reach their ends.
All inputs are finite; a program needn't handle non-finite values. Where the reference program divides by a largest or mean magnitude, that divisor is 1e-20 or more. No bound on the sum of `wall_types` on one device may be relied on, other than what follows from the above.
Results may differ from the reference program's by a relative error of at most 0.0003.
Values sent between devices are 32-bit elements; how exact they have to be, the bound alone decides.
No kernel may reach another device: no remote copies, remote signals or barrier semaphores. Data moves between devices by JAX's collectives and lax.ppermute only.
A program may use at most 64 MiB of HBM per device.

```python
import math
import jax
import jax.numpy as jnp
from jax import lax

SPECIES = 5
P_SIZE = 4
ITERS = 2
NX = 2
NY = 8
NZ = 128
MX = 8
MY = 32
MZ = 512


def element_factor(key, lowest):
    values = jax.random.uniform(key, (NX, NY, NZ), jnp.float32, math.log(lowest), 0.0)
    values = jnp.exp(values)
    values = jnp.repeat(values, P_SIZE, axis=0)
    values = jnp.repeat(values, P_SIZE, axis=1)
    return jnp.repeat(values, P_SIZE, axis=2)


def node_factor(key, shape, lowest, highest):
    logs = jax.random.uniform(key, shape, jnp.float32, math.log(lowest), math.log(highest))
    return jnp.exp(logs)


def draw_species(key, part):
    factor = element_factor(jax.random.fold_in(key, 11), 0.3)
    nodes = node_factor(jax.random.fold_in(key, 12), (SPECIES, MX, MY, MZ), 0.3, 0.6)
    return (nodes * factor[None]).astype(jnp.float32)


def draw_pressure_in(key, part):
    factor = element_factor(jax.random.fold_in(key, 21), 0.25)
    nodes = node_factor(jax.random.fold_in(key, 22), (MX, MY, MZ), 0.5, 1.0)
    return (nodes * factor).astype(jnp.float32)


def set_ends(drawn, own_key, least, largest):
    shape = drawn.shape
    place = [jax.random.randint(jax.random.fold_in(own_key, axis), (), 0, shape[axis]) for axis in range(len(shape))]
    drawn = drawn.at[tuple(place)].set(least)
    longest = shape.index(max(shape))
    place[longest] = (place[longest] + 1) % shape[longest]
    return drawn.at[tuple(place)].set(largest)


def levels(key, shape, pieces, least, high):
    def one(dim, blocks):
        heights = jax.random.uniform(jax.random.fold_in(jax.random.fold_in(key, 6), dim), (blocks,), jnp.float32, least / len(pieces), high / len(pieces))
        return jnp.repeat(jnp.exp(heights), shape[dim] // blocks).reshape((-1,) + (1,) * (len(shape) - dim - 1))

    gain = one(*pieces[0])
    for cut in pieces[1:]:
        gain = gain * one(*cut)
    return gain


def bell_draw(own_key, shape, deviation, limit, shards=(), held_as=jnp.bfloat16):
    entries = jax.random.normal(own_key, shape, jnp.float32) * deviation
    if len(shards) > 0:
        entries = levels(own_key, shape, shards, -0.22, 0.18) * entries
    return jnp.clip(entries, min=-limit, max=limit).astype(held_as)


def setup_inputs(seed: int = 0) -> dict:
    seeds = jax.random.split(jax.random.key(seed), 5)
    species = draw_species(jax.random.fold_in(seeds[4], 71), 0)
    velocity_in = bell_draw(seeds[1], (3, MX, MY, MZ), 0.5, 3.0, ((1, 2), (2, 4), (3, 4)), jnp.float32)
    pressure_in = draw_pressure_in(jax.random.fold_in(seeds[4], 71), 0)
    wall_types = set_ends((jax.random.randint(seeds[3], (3, NX, NY, NZ), 0, 4) < 1).astype(jnp.int32), jax.random.fold_in(seeds[3], 1), 0, 1)
    return {"species": species, "velocity_in": velocity_in, "pressure_in": pressure_in, "wall_types": wall_types}


GAMMA = 1.4
COURANT = 0.4
FLOOR = 0.1
SLOPE_FLOOR = 0.01
SPREAD = 0.002
RELAX = 0.1

def primitives(conserved):
    density = lax.optimization_barrier(jnp.sum(conserved[:SPECIES], axis=0))
    safe_rho = jnp.maximum(density, FLOOR)
    momentum = conserved[SPECIES:SPECIES + 3]
    velocity = momentum / safe_rho
    pressure = (GAMMA - 1.0) * (conserved[SPECIES + 3] - 0.5 * lax.optimization_barrier(jnp.sum(momentum * velocity, axis=0)))
    sound = jnp.sqrt(GAMMA * jnp.maximum(pressure, FLOOR) / safe_rho)
    return (density, safe_rho, velocity, pressure, sound)

def entropy(density, safe_rho, pressure):
    return density * (jnp.log(jnp.maximum(pressure, FLOOR)) - GAMMA * jnp.log(safe_rho))

def component_mask(target, length):
    component = lax.broadcasted_iota(jnp.int32, (length, 1, 1, 1), 0)
    return component == target

def node_flux(conserved, velocity, pressure, spatial):
    along = velocity[spatial]
    length = conserved.shape[0]
    normal = component_mask(SPECIES + spatial, length)
    energy_row = component_mask(SPECIES + 3, length)
    return conserved * along + jnp.where(normal, pressure, 0.0) + jnp.where(energy_row, pressure * along, 0.0)

def element_form(values):
    blocks = [extent // P_SIZE for extent in values.shape]
    return values.reshape(blocks[0], P_SIZE, blocks[1], P_SIZE, blocks[2], P_SIZE)

def element_min(values):
    return lax.optimization_barrier(jnp.min(element_form(values), axis=(1, 3, 5)))

def element_mean(values):
    return lax.optimization_barrier(jnp.mean(element_form(values), axis=(1, 3, 5)))

def to_nodes(values):
    blocks = values.shape
    wide = jnp.broadcast_to(values[:, None, :, None, :, None], (blocks[0], P_SIZE, blocks[1], P_SIZE, blocks[2], P_SIZE))
    return wide.reshape(blocks[0] * P_SIZE, blocks[1] * P_SIZE, blocks[2] * P_SIZE)

def neighbour_min(values):
    result = values
    for spatial in range(3):
        result = jnp.minimum(result, jnp.roll(values, 1, spatial))
        result = jnp.minimum(result, jnp.roll(values, -1, spatial))
    return result

def interface_pair(conserved, velocity, pressure, sound, wall_types, spatial):
    array_axis = spatial + 1
    terms = node_flux(conserved, velocity, pressure, spatial)
    right_terms = jnp.roll(terms, -1, array_axis)
    high_flux = (7.0 * (terms + right_terms) - (jnp.roll(terms, 1, array_axis) + jnp.roll(terms, -2, array_axis))) / 12.0
    wave_rate = jnp.abs(velocity[spatial]) + sound
    max_rate = jnp.maximum(wave_rate, jnp.roll(wave_rate, -1, spatial))
    low_flux = 0.5 * (terms + right_terms) - 0.5 * max_rate * (jnp.roll(conserved, -1, array_axis) - conserved)
    wall_flux = jnp.where(component_mask(SPECIES + spatial, conserved.shape[0]), 0.5 * (pressure + jnp.roll(pressure, -1, spatial)), 0.0)
    position = lax.broadcasted_iota(jnp.int32, pressure.shape, spatial)
    wall_flags = jnp.roll(to_nodes(wall_types[spatial]), -1, spatial)
    wall_face = (position % P_SIZE == P_SIZE - 1) & (wall_flags == 1)
    return (jnp.where(wall_face, wall_flux, low_flux), jnp.where(wall_face, wall_flux, high_flux))

def divergence(fluxes):
    result = fluxes[0] - jnp.roll(fluxes[0], 1, 1)
    for spatial in range(1, 3):
        result = result + fluxes[spatial] - jnp.roll(fluxes[spatial], 1, spatial + 1)
    return result

def newton_update(blending, delta, trial_rho, trial_vel, trial_p, residual, rho_bound, p_bound, lowest, mean_sq):
    node_blend = to_nodes(blending)
    rho_target = rho_bound - RELAX * jnp.maximum(rho_bound - lowest[0], 0.0)
    p_target = p_bound - RELAX * jnp.maximum(p_bound - lowest[1], 0.0)
    d_rho = lax.optimization_barrier(jnp.sum(delta[:SPECIES], axis=0))
    slope = (GAMMA - 1.0) * (delta[SPECIES + 3] - lax.optimization_barrier(jnp.sum(trial_vel * delta[SPECIES:SPECIES + 3], axis=0)) + 0.5 * lax.optimization_barrier(jnp.sum(trial_vel * trial_vel, axis=0)) * d_rho)
    t_rho = node_blend + jnp.minimum(trial_rho - to_nodes(rho_target), 0.0) / jnp.maximum(-d_rho, SLOPE_FLOOR)
    t_pres = node_blend + jnp.minimum(trial_p - to_nodes(p_target), 0.0) / jnp.maximum(-slope, SLOPE_FLOOR)
    cap = (mean_sq + SPREAD) / (mean_sq + SPREAD + element_mean(residual * residual))
    return jnp.maximum(jnp.minimum(cap, jnp.minimum(element_min(t_rho), element_min(t_pres))), 0.0)

def reference(species, velocity_in, pressure_in, wall_types):
    density_in = lax.optimization_barrier(jnp.sum(species, axis=0))
    momentum = density_in * velocity_in
    energy = pressure_in / (GAMMA - 1.0) + 0.5 * density_in * lax.optimization_barrier(jnp.sum(velocity_in * velocity_in, axis=0))
    conserved = jnp.concatenate([species, momentum, energy[None]], axis=0)
    density, safe_rho, velocity, pressure, sound = primitives(conserved)
    speed_max = jnp.max(lax.optimization_barrier(jnp.sum(jnp.abs(velocity), axis=0)) + 3.0 * sound)
    step_ratio = COURANT / speed_max
    flux_pairs = [interface_pair(conserved, velocity, pressure, sound, wall_types, spatial) for spatial in range(3)]
    low_state = conserved - step_ratio * divergence([pair[0] for pair in flux_pairs])
    high_state = conserved - step_ratio * divergence([pair[1] for pair in flux_pairs])
    delta = high_state - low_state
    rho_bound = neighbour_min(element_min(density))
    p_bound = neighbour_min(element_min(pressure))
    low_prims = primitives(low_state)
    low_sigma = entropy(low_prims[0], low_prims[1], low_prims[3])
    blending = jnp.ones(rho_bound.shape, jnp.float32)
    for newton in range(ITERS):
        trial_state = low_state + to_nodes(blending) * delta
        trial_prims = primitives(trial_state)
        residual = entropy(trial_prims[0], trial_prims[1], trial_prims[3]) - low_sigma
        lowest = jnp.stack([jnp.min(trial_prims[0]), jnp.min(trial_prims[3])])
        mean_sq = jnp.sum(residual * residual) / residual.size
        blending = newton_update(blending, delta, trial_prims[0], trial_prims[2], trial_prims[3], residual, rho_bound, p_bound, lowest, mean_sq)
    node_blend = to_nodes(blending)
    blended = []
    for spatial in range(3):
        face_theta = jnp.minimum(node_blend, jnp.roll(node_blend, -1, spatial))
        low_flux, high_flux = flux_pairs[spatial]
        blended.append(low_flux + face_theta * (high_flux - low_flux))
    new_state = conserved - step_ratio * divergence(blended)
    return (new_state, blending)
```

```python
import jax
import jax.numpy as jnp
from jax import lax
from jax.experimental import pallas as pl
from jax.experimental.pallas import tpu as pltpu
from jax.sharding import PartitionSpec as P

SPECIES = 5
COMPS = SPECIES + 4
P_SIZE = 4
HALO = 2
AXES = ("gx", "gy", "gz")

GAMMA = 1.4
COURANT = 0.4
FLOOR = 0.1
SLOPE_FLOOR = 0.01
SPREAD = 0.002
RELAX = 0.1


def ids(shape, axis):
    return lax.broadcasted_iota(jnp.int32, shape, axis)


def turn(values, shift, axis):
    extent = values.shape[axis]
    shift = shift % extent
    if shift == 0:
        return values
    return pltpu.roll(values, shift, axis)


def group(values, axis, combine):
    place = ids(values.shape, axis)
    step = 1
    while step < P_SIZE:
        other = jnp.where((place & step) == 0, turn(values, -step, axis), turn(values, step, axis))
        values = combine(values, other)
        step *= 2
    return values


def element(values, combine):
    return group(group(values, 0, combine), 1, combine)


def primitives(density, momentum, energy):
    safe = jnp.maximum(density, FLOOR)
    inverse = 1.0 / safe
    velocity = [m * inverse for m in momentum]
    kinetic = momentum[0] * velocity[0] + momentum[1] * velocity[1] + momentum[2] * velocity[2]
    pressure = (GAMMA - 1.0) * (energy - 0.5 * kinetic)
    return safe, inverse, velocity, pressure


def state_primitives(conserved):
    density = conserved[0]
    for c in range(1, SPECIES):
        density = density + conserved[c]
    _, inverse, velocity, pressure = primitives(
        density, conserved[SPECIES : SPECIES + 3], conserved[SPECIES + 3]
    )
    sound = jnp.sqrt(GAMMA * jnp.maximum(pressure, FLOOR) * inverse)
    return density, velocity, pressure, sound


def entropy(density, safe, pressure):
    return density * (jnp.log(jnp.maximum(pressure, FLOOR)) - GAMMA * jnp.log(safe))


def next_along(values, after, axis, step=1):
    place = ids(values.shape, axis)
    return turn(jnp.where(place < step, after, values), -step, axis)


def previous_along(values, before, axis, step=1):
    extent = values.shape[axis]
    place = ids(values.shape, axis)
    return turn(jnp.where(place >= extent - step, before, values), step, axis)


def pack_kernel(zdim, sp_ref, vel_ref, p_ref, wall_ref, x_ref, up_ref, down_ref, z_ref, own_ref):
    nx, ny, nz = p_ref.shape
    species = [sp_ref[c] for c in range(SPECIES)]
    speed_in = [vel_ref[d] for d in range(3)]
    density_in = species[0]
    for c in range(1, SPECIES):
        density_in = density_in + species[c]
    square = speed_in[0] * speed_in[0] + speed_in[1] * speed_in[1] + speed_in[2] * speed_in[2]
    energy = p_ref[...] / (GAMMA - 1.0) + 0.5 * density_in * square
    conserved = species + [density_in * v for v in speed_in] + [energy]
    density, velocity, pressure, sound = state_primitives(conserved)
    speed = jnp.abs(velocity[0]) + jnp.abs(velocity[1]) + jnp.abs(velocity[2]) + 3.0 * sound
    top = jnp.max(jnp.max(speed, axis=0), keepdims=True)
    rho_min = element(jnp.min(density, axis=0), jnp.minimum)
    p_min = element(jnp.min(pressure, axis=0), jnp.minimum)

    ney, nez = wall_ref.shape[2:]
    spread = (ids((nez, nz), 0) == ids((nez, nz), 1) // P_SIZE).astype(jnp.float32)
    rows = ids((ny, nz), 0)
    lanes = ids((ny, nz), 1)
    walls = []
    for d in range(3):
        wide = jnp.dot(
            wall_ref[d, 0].astype(jnp.float32), spread, preferred_element_type=jnp.float32
        )
        flags = jnp.broadcast_to(wide[0:1], (ny, nz))
        for e in range(1, ney):
            flags = jnp.where(rows >= e * P_SIZE, jnp.broadcast_to(wide[e : e + 1], (ny, nz)), flags)
        walls.append(flags)

    for c in range(COMPS):
        x_ref[c] = conserved[c]
    x_ref[COMPS, 0] = rho_min
    x_ref[COMPS, 1] = p_min
    x_ref[COMPS, 2] = walls[0]
    for x in range(3, nx):
        x_ref[COMPS, x] = walls[0]
    own_ref[0] = walls[1]
    own_ref[1] = walls[2]

    for c in range(COMPS):
        for x in range(nx):
            plane = conserved[c][x]
            up_ref[c, HALO * x : HALO * (x + 1), :] = plane[ny - HALO : ny, :]
            down_ref[c, HALO * x : HALO * (x + 1), :] = plane[0:HALO, :]
    for ref, row in ((up_ref, ny - 1), (down_ref, 0)):
        extra = jnp.where(rows == 0, rho_min[row : row + 1], p_min[row : row + 1])
        ref[COMPS] = jnp.where(rows == 2, walls[1][row : row + 1], extra)

    first = jnp.zeros((ny, nz), jnp.float32)
    last = first
    for c in range(COMPS):
        for x in range(nx):
            slot = c * nx + x
            here = lanes // HALO == slot
            plane = conserved[c][x]
            first = jnp.where(here, turn(plane, HALO * slot, 1), first)
            last = jnp.where(here, turn(plane, HALO * slot + HALO, 1), last)
    spare = HALO * COMPS * nx
    packed = []
    for base, lane in ((first, 0), (last, nz - 1)):
        for i, value in enumerate((rho_min, p_min, walls[2])):
            base = jnp.where(lanes == spare + i, value[:, lane : lane + 1], base)
        packed.append(jnp.where(lanes == spare + 3, top, base))
    first, last = packed
    count = z_ref.shape[0]
    follow = lax.rem(lax.axis_index("gz") + 1, zdim)
    to_next = ids((count, 1, 1), 0) % zdim == follow
    z_ref[...] = jnp.where(to_next, last[None], first[None])


def neighbours(zdim):
    me = lax.axis_index("gz")
    base = (lax.axis_index("gx") * lax.axis_size("gy") + lax.axis_index("gy")) * zdim
    return base + lax.rem(me + zdim - 1, zdim), base + lax.rem(me + 1, zdim)


def state_kernel(
    zdim, xcount, x_ref, own_ref, *refs
):
    x_halo = refs[:xcount]
    below_ref, above_ref, z_ref = refs[xcount : xcount + 3]
    low_ref, dx_ref, dy_ref, dz_ref, it_ref, el_ref, stat_ref = refs[xcount + 3 :]
    _, nx, ny, nz = x_ref.shape
    shape = (nx, ny, nz)
    before_ref, after_ref = x_halo[0], x_halo[-1]
    rows = ids((ny, nz), 0)
    lanes = ids((ny, nz), 1)
    zlow, zhigh = neighbours(zdim)
    zbelow = z_ref[zlow]
    zabove = z_ref[zhigh]
    count = z_ref.shape[0]
    spare = HALO * COMPS * nx
    speed = jnp.max(z_ref[...], axis=0)[:, spare + 3 : spare + 4]
    ratio = COURANT / jnp.broadcast_to(speed, (ny, nz))

    own = [x_ref[c] for c in range(COMPS)]
    density, velocity, pressure, sound = state_primitives(own)
    low_sum = [None] * COMPS
    delta_sum = [None] * COMPS
    rho_bound = x_ref[COMPS, 0]
    p_bound = x_ref[COMPS, 1]
    bounds = [rho_bound, p_bound]

    def add(total, value):
        return value if total is None else total + value

    halo = [
        jnp.concatenate([before_ref[c, nx - HALO : nx], after_ref[c, 0:HALO]], axis=0)
        for c in range(COMPS)
    ]
    _, h_velocity, h_pressure, h_sound = state_primitives(halo)

    def wide(inner, outer):
        return jnp.concatenate([outer[0:HALO], inner, outer[HALO : 2 * HALO]], axis=0)

    along = wide(velocity[0], h_velocity[0])
    press = wide(pressure, h_pressure)
    rate = jnp.abs(along) + wide(sound, h_sound)
    faces = nx + 1
    half_rate = 0.5 * jnp.maximum(rate[1 : 1 + faces], rate[2 : 2 + faces])
    flags = jnp.concatenate(
        [x_ref[COMPS, 2][None], jnp.zeros((nx - 1, ny, nz), jnp.float32), after_ref[COMPS, 2][None]],
        axis=0,
    )
    wall = flags > 0.5
    for c in range(COMPS):
        cons = wide(own[c], halo[c])
        term = cons * along
        if c == SPECIES:
            term = term + press
        if c == SPECIES + 3:
            term = term + press * along
        pair = term[1 : 1 + faces] + term[2 : 2 + faces]
        outer = term[0:faces] + term[3 : 3 + faces]
        drop = half_rate * (cons[2 : 2 + faces] - cons[1 : 1 + faces])
        low = 0.5 * pair - drop
        gap = (pair - outer) * (1.0 / 12.0) + drop
        if c == SPECIES:
            low = jnp.where(wall, 0.5 * (press[1 : 1 + faces] + press[2 : 2 + faces]), low)
        else:
            low = jnp.where(wall, 0.0, low)
        gap = jnp.where(wall, 0.0, gap)
        dx_ref[c] = gap
        low_sum[c] = low[1:faces] - low[0:nx]
        delta_sum[c] = gap[1:faces] - gap[0:nx]
    for i in range(2):
        bounds[i] = jnp.minimum(bounds[i], before_ref[COMPS, i])
        bounds[i] = jnp.minimum(bounds[i], after_ref[COMPS, i])

    for d in (1, 2):
        axis = d - 1
        place = rows if d == 1 else lanes
        extent = ny if d == 1 else nz
        halo = []
        for c in range(COMPS):
            made = []
            for x in range(nx):
                if d == 1:
                    after = turn(above_ref[c], -HALO * x, 0)
                    before = turn(below_ref[c], ny - HALO - HALO * x, 0)
                else:
                    slot = c * nx + x
                    after = turn(zabove, -HALO * slot, 1)
                    before = turn(zbelow, nz - HALO - HALO * slot, 1)
                made.append(jnp.where(place < HALO, after, before)[None])
            halo.append(jnp.concatenate(made, axis=0))
        _, h_velocity, h_pressure, h_sound = state_primitives(halo)
        full = ids(shape, d)

        def plus(values, outside, step):
            return turn(jnp.where(full < step, outside, values), -step, d)

        def minus(values, outside, step):
            return turn(jnp.where(full >= extent - step, outside, values), step, d)

        along, h_along = velocity[d], h_velocity[d]
        rate = jnp.abs(along) + sound
        h_rate = jnp.abs(h_along) + h_sound
        rate_up = 0.5 * jnp.maximum(rate, plus(rate, h_rate, 1))
        rate_down = 0.5 * jnp.maximum(minus(rate, h_rate, 1), rate)
        press_up = 0.5 * (pressure + plus(pressure, h_pressure, 1))
        press_down = 0.5 * (minus(pressure, h_pressure, 1) + pressure)
        mine = own_ref[axis]
        if d == 1:
            theirs = jnp.broadcast_to(above_ref[COMPS, 2:3, :], (ny, nz))
        else:
            theirs = jnp.broadcast_to(zabove[:, spare + 2 : spare + 3], (ny, nz))
        flag_up = (place % P_SIZE == P_SIZE - 1) & (next_along(mine, theirs, axis) > 0.5)
        flag_down = (place % P_SIZE == 0) & (mine > 0.5)
        wall_up = jnp.broadcast_to(jnp.where(flag_up, 1.0, 0.0)[None], shape) > 0.5
        wall_down = jnp.broadcast_to(jnp.where(flag_down, 1.0, 0.0)[None], shape) > 0.5
        out_ref = dy_ref if d == 1 else dz_ref
        for c in range(COMPS):
            term = own[c] * along
            h_term = halo[c] * h_along
            if c == SPECIES + d:
                term = term + pressure
                h_term = h_term + h_pressure
            if c == SPECIES + 3:
                term = term + pressure * along
                h_term = h_term + h_pressure * h_along
            ahead = plus(term, h_term, 1)
            ahead2 = plus(term, h_term, 2)
            back = minus(term, h_term, 1)
            back2 = minus(term, h_term, 2)
            pair_up = term + ahead
            pair_down = back + term
            drop_up = rate_up * (plus(own[c], halo[c], 1) - own[c])
            drop_down = rate_down * (own[c] - minus(own[c], halo[c], 1))
            low_up = 0.5 * pair_up - drop_up
            low_down = 0.5 * pair_down - drop_down
            gap_up = (pair_up - (back + ahead2)) * (1.0 / 12.0) + drop_up
            gap_down = (pair_down - (back2 + ahead)) * (1.0 / 12.0) + drop_down
            low_up = jnp.where(wall_up, press_up if c == SPECIES + d else 0.0, low_up)
            low_down = jnp.where(wall_down, press_down if c == SPECIES + d else 0.0, low_down)
            gap_up = jnp.where(wall_up, 0.0, gap_up)
            gap_down = jnp.where(wall_down, 0.0, gap_down)
            out_ref[0, c] = gap_down
            out_ref[1, c] = gap_up
            low_sum[c] = low_sum[c] + (low_up - low_down)
            delta_sum[c] = delta_sum[c] + (gap_up - gap_down)
        for i in range(2):
            base = x_ref[COMPS, i]
            if d == 1:
                after = jnp.broadcast_to(above_ref[COMPS, i : i + 1, :], (ny, nz))
                before = jnp.broadcast_to(below_ref[COMPS, i : i + 1, :], (ny, nz))
            else:
                after = jnp.broadcast_to(zabove[:, spare + i : spare + i + 1], (ny, nz))
                before = jnp.broadcast_to(zbelow[:, spare + i : spare + i + 1], (ny, nz))
            bounds[i] = jnp.minimum(bounds[i], next_along(base, after, axis, P_SIZE))
            bounds[i] = jnp.minimum(bounds[i], previous_along(base, before, axis, P_SIZE))

    scale = ratio[None]
    low = []
    delta = []
    for c in range(COMPS):
        value = own[c] - scale * low_sum[c]
        low_ref[c] = value
        low.append(value)
        delta.append(-scale * delta_sum[c])

    def reduced(values):
        total = values[0]
        for c in range(1, SPECIES):
            total = total + values[c]
        return [total] + values[SPECIES:]

    low = reduced(low)
    delta = reduced(delta)
    safe, _, _, low_p = primitives(low[0], low[1:4], low[4])
    low_sigma = entropy(low[0], safe, low_p)
    trial = [a + b for a, b in zip(low, delta)]
    rho, press, square, slope = trial_values(trial, delta, low_sigma)
    for i in range(5):
        it_ref[i] = low[i]
        it_ref[5 + i] = delta[i]
    it_ref[10] = low_sigma
    it_ref[11] = rho
    it_ref[12] = press
    it_ref[13] = 1.0 / jnp.maximum(-delta[0], SLOPE_FLOOR)
    it_ref[14] = 1.0 / jnp.maximum(-slope, SLOPE_FLOOR)
    el_ref[0] = bounds[0]
    el_ref[1] = bounds[1]
    el_ref[2] = mean_over_element(square)
    el_ref[3] = ratio
    row = ids((1, nz), 1)
    stat = jnp.where(
        row == 0,
        jnp.min(jnp.min(rho, axis=0), keepdims=True),
        jnp.where(
            row == 1,
            jnp.min(jnp.min(press, axis=0), keepdims=True),
            jnp.sum(jnp.sum(square, axis=0), keepdims=True),
        ),
    )
    stat_ref[...] = jnp.broadcast_to(stat, (count, nz))


def trial_values(trial, delta, low_sigma):
    safe, _, velocity, press = primitives(trial[0], trial[1:4], trial[4])
    residual = entropy(trial[0], safe, press) - low_sigma
    turned = velocity[0] * delta[1] + velocity[1] * delta[2] + velocity[2] * delta[3]
    speed = velocity[0] * velocity[0] + velocity[1] * velocity[1] + velocity[2] * velocity[2]
    slope = (GAMMA - 1.0) * (delta[4] - turned + 0.5 * speed * delta[0])
    return trial[0], press, residual * residual, slope


def mean_over_element(square):
    nodes = P_SIZE * P_SIZE * P_SIZE
    return element(jnp.sum(square, axis=0), jnp.add) * (1.0 / nodes)


def new_blending(lowest_rho, lowest_p, mean_sq, before, rho, press, rho_rate, p_rate, rho_bound, p_bound, spread):
    rho_target = rho_bound - RELAX * jnp.maximum(rho_bound - lowest_rho, 0.0)
    p_target = p_bound - RELAX * jnp.maximum(p_bound - lowest_p, 0.0)
    t_rho = jnp.minimum(rho - rho_target[None], 0.0) * rho_rate
    t_p = jnp.minimum(press - p_target[None], 0.0) * p_rate
    least = before + jnp.min(jnp.minimum(t_rho, t_p), axis=0)
    least = element(least, jnp.minimum)
    cap = (mean_sq + SPREAD) / (mean_sq + SPREAD + spread)
    return jnp.maximum(jnp.minimum(cap, least), 0.0)


def newton_kernel(zdim, nodes, it_ref, el_ref, stat_ref, g_ref, z_ref):
    _, nx, ny, nz = it_ref.shape
    stats = stat_ref[...]
    least = jnp.min(stats, axis=0, keepdims=True)
    total = jnp.sum(stats, axis=0, keepdims=True)
    mean_sq = total[:, 2:3] * (1.0 / nodes)
    theta = new_blending(
        least[:, 0:1], least[:, 1:2], mean_sq, 1.0,
        it_ref[11], it_ref[12], it_ref[13], it_ref[14], el_ref[0], el_ref[1], el_ref[2],
    )
    low = [it_ref[i] for i in range(5)]
    delta = [it_ref[5 + i] for i in range(5)]
    trial = [a + theta[None] * b for a, b in zip(low, delta)]
    rho, press, square, slope = trial_values(trial, delta, it_ref[10])
    extras = (el_ref[0], el_ref[1], theta, mean_over_element(square))
    fields = [rho, press, it_ref[13], 1.0 / jnp.maximum(-slope, SLOPE_FLOOR)]
    planes = []
    for f in range(4):
        g_ref[f] = fields[f]
        planes += [fields[f][x] for x in range(nx)]
    for i in range(4):
        g_ref[4, i] = extras[i]
    planes += list(extras)
    lanes = ids((ny, nz), 1)
    first = jnp.zeros((ny, nz), jnp.float32)
    last = first
    for slot, plane in enumerate(planes):
        here = lanes // P_SIZE == slot
        first = jnp.where(here, turn(plane, P_SIZE * slot, 1), first)
        last = jnp.where(here, turn(plane, P_SIZE * slot + P_SIZE, 1), last)
    spare = P_SIZE * len(planes)
    stats = (
        jnp.min(jnp.min(rho, axis=0), keepdims=True),
        jnp.min(jnp.min(press, axis=0), keepdims=True),
        jnp.sum(jnp.sum(square, axis=0), keepdims=True),
    )
    for i, value in enumerate(stats):
        first = jnp.where(lanes == spare + i, value, first)
        last = jnp.where(lanes == spare + i, value, last)
    count = z_ref.shape[0]
    follow = lax.rem(lax.axis_index("gz") + 1, zdim)
    to_next = ids((count, 1, 1), 0) % zdim == follow
    z_ref[...] = jnp.where(to_next, last[None], first[None])


def final_kernel(zdim, nodes, xcount, g_ref, low_ref, dx_ref, dy_ref, dz_ref, el_ref, *refs):
    x_halo = refs[:xcount]
    below_ref, above_ref, z_ref, new_ref, blend_ref = refs[xcount:]
    _, nx, ny, nz = g_ref.shape
    rows = ids((ny, nz), 0)
    lanes = ids((ny, nz), 1)
    zlow, zhigh = neighbours(zdim)
    zbelow = z_ref[zlow]
    zabove = z_ref[zhigh]
    slots = 4 * nx + 4
    spare = P_SIZE * slots
    every = z_ref[...]
    least = jnp.min(every, axis=0)
    total = jnp.sum(every, axis=0)
    lowest_rho = least[:, spare : spare + 1]
    lowest_p = least[:, spare + 1 : spare + 2]
    mean_sq = total[:, spare + 2 : spare + 3] * (1.0 / nodes)

    def blending(fields, extras):
        return new_blending(
            lowest_rho, lowest_p, mean_sq, extras[2], fields[0], fields[1], fields[2], fields[3],
            extras[0], extras[1], extras[3],
        )

    def of_block(ref):
        return blending([ref[f] for f in range(4)], [ref[4, i] for i in range(4)])

    theta = of_block(g_ref)
    x_theta = [of_block(ref) for ref in x_halo]
    below = of_block(below_ref)
    above = of_block(above_ref)
    strip = [
        jnp.where(
            lanes < P_SIZE,
            turn(zabove, -P_SIZE * slot, 1),
            turn(zbelow, nz - P_SIZE - P_SIZE * slot, 1),
        )
        for slot in range(slots)
    ]
    beside = blending(
        [jnp.stack(strip[f * nx : (f + 1) * nx], axis=0) for f in range(4)], strip[4 * nx :]
    )
    x_down = jnp.minimum(theta, x_theta[0])
    x_up = jnp.minimum(theta, x_theta[-1])
    y_down = jnp.minimum(theta, previous_along(theta, below, 0))[None]
    y_up = jnp.minimum(theta, next_along(theta, above, 0))[None]
    z_down = jnp.minimum(theta, previous_along(theta, beside, 1))[None]
    z_up = jnp.minimum(theta, next_along(theta, beside, 1))[None]
    x_face = jnp.stack([x_down] + [theta] * (nx - 1) + [x_up], axis=0)
    ratio = el_ref[3][None]
    for c in range(COMPS):
        x_part = x_face * dx_ref[c]
        change = x_part[1 : nx + 1] - x_part[0:nx]
        change = change + (y_up * dy_ref[1, c] - y_down * dy_ref[0, c])
        change = change + (z_up * dz_ref[1, c] - z_down * dz_ref[0, c])
        new_ref[c] = low_ref[c] - ratio * change
    _, ney, nez = blend_ref.shape
    pick = (ids((nz, nez), 0) == ids((nz, nez), 1) * P_SIZE).astype(jnp.float32)
    narrow = jnp.dot(
        theta, pick, preferred_element_type=jnp.float32, precision=lax.Precision.HIGHEST
    )
    for e in range(ney):
        blend_ref[0, e : e + 1, :] = narrow[e * P_SIZE : e * P_SIZE + 1, :]


def ring(axis, step):
    count = lax.axis_size(axis)
    return [(i, (i + step) % count) for i in range(count)]


def swap_x(block):
    from_before = lax.ppermute(block, "gx", ring("gx", 1))
    if lax.axis_size("gx") == 2:
        return [from_before]
    return [from_before, lax.ppermute(block, "gx", ring("gx", -1))]


def call(body, out_shapes, *args):
    vmem = pl.BlockSpec(memory_space=pltpu.VMEM)
    return pl.pallas_call(
        body,
        out_shape=[jax.ShapeDtypeStruct(s, jnp.float32) for s in out_shapes],
        in_specs=[vmem] * len(args),
        out_specs=[vmem] * len(out_shapes),
    )(*args)


def local(species, velocity_in, pressure_in, wall_types):
    nx, ny, nz = pressure_in.shape
    zdim = lax.axis_size("gz")
    count = lax.axis_size("gx") * lax.axis_size("gy") * zdim
    nodes = nx * ny * nz * count
    if nx != P_SIZE or HALO * nx != ny or HALO * COMPS * nx + 4 > nz or zdim < 3:
        raise ValueError("unsupported block")

    def pack(*refs):
        pack_kernel(zdim, *refs)

    x_send, up_send, down_send, z_send, own = call(
        pack,
        [(COMPS + 1, nx, ny, nz), (COMPS + 1, ny, nz), (COMPS + 1, ny, nz), (count, ny, nz), (2, ny, nz)],
        species, velocity_in, pressure_in, wall_types,
    )
    x_halo = swap_x(x_send)
    below = lax.ppermute(up_send, "gy", ring("gy", 1))
    above = lax.ppermute(down_send, "gy", ring("gy", -1))
    z_got = lax.all_to_all(z_send, AXES, 0, 0, tiled=True)

    def state(*refs):
        state_kernel(zdim, len(x_halo), *refs)

    low, dx, dy, dz, it, el, stat = call(
        state,
        [
            (COMPS, nx, ny, nz), (COMPS, nx + 1, ny, nz), (2, COMPS, nx, ny, nz), (2, COMPS, nx, ny, nz),
            (15, nx, ny, nz), (4, ny, nz), (count, nz),
        ],
        x_send, own, *x_halo, below, above, z_got,
    )
    stats = lax.all_to_all(stat, AXES, 0, 0, tiled=True)

    def newton(*refs):
        newton_kernel(zdim, nodes, *refs)

    g_send, zg_send = call(newton, [(5, nx, ny, nz), (count, ny, nz)], it, el, stats)
    gx_halo = swap_x(g_send)
    g_below = lax.ppermute(g_send, "gy", ring("gy", 1))
    g_above = lax.ppermute(g_send, "gy", ring("gy", -1))
    zg_got = lax.all_to_all(zg_send, AXES, 0, 0, tiled=True)

    def final(*refs):
        final_kernel(zdim, nodes, len(gx_halo), *refs)

    new_state, blending = call(
        final,
        [(COMPS, nx, ny, nz), wall_types.shape[1:]],
        g_send, low, dx, dy, dz, el, *gx_halo, g_below, g_above, zg_got,
    )
    return new_state, blending


def solution(mesh):
    in_specs = (
        P(None, "gx", "gy", "gz"),
        P(None, "gx", "gy", "gz"),
        P("gx", "gy", "gz"),
        P(None, "gx", "gy", "gz"),
    )
    out_specs = (P(None, "gx", "gy", "gz"), P("gx", "gy", "gz"))
    return jax.shard_map(local, mesh=mesh, in_specs=in_specs, out_specs=out_specs, check_vma=False)
```
